32 devices in a mesh: parts: 2 (over y), ep: 16 (over z, x, core).
Axes of the slice: x: 2, y: 2, z: 4, core: 2. Of those that a mesh axis runs over, the one named last changes fastest.
Arguments:
- tokens: bfloat16 [512, 2048], P(('parts', 'ep')), parts along dimension 0, may hold values from -6 to 6
- gate_up: bfloat16 [4096, 16, 1536], P(('parts', 'ep')), parts along dimension 0, may hold values from -0.125 to 0.125
- down_proj: bfloat16 [1536, 16, 2048], P(('parts', 'ep')), parts along dimension 0, may hold values from -0.21875 to 0.21875
- expert_ids: int32 [512, 8], P(('parts', 'ep')), parts along dimension 0, may hold values from 0 to 15, all different within a row; in each aligned block of 16 rows (0 to 15, 16 to 31, ...) at most 16 rows name the same one
- gate_weights: float32 [512, 8], P(('parts', 'ep')), parts along dimension 0, may hold values from 0.03 to 0.6
- owner_slot: int32 [32], P('parts'), parts along dimension 0, may hold values from 0 to 15, each once
Outputs:
- moe_out: bfloat16 [512, 2048], P(('parts', 'ep')), parts along dimension 0
- channel_scale: float32 [32, 3584], P(('parts', 'ep')), parts along dimension 0
The draws below stay inside these ranges and needn't reach their ends.
There are 2 independent parts, one for each index of `parts`. The reference program is written for one: setup_inputs(seed, part) draws one part's arguments, and reference() takes and returns one part's arrays. A program takes and returns all parts, laid end to end along the dimension named above; each array names one. Nothing has to cross between parts.
Inputs may be any that keep to these rules, and one draw needn't show every extreme that they name: `expert_ids`: each row names 8 different experts; among the rows of one device no expert is named more than 16 times, a bound that some block reaches. `owner_slot`: A permutation: each slot holds exactly one expert.
All inputs are finite; a program needn't handle non-finite values.
Results may differ from the reference program's by a relative error of at most 0.0058.
Values may be sent and summed in bfloat16 or wider, within the bound.
A program may use at most 128 MiB of HBM per device.

```python
import math
import jax
import jax.numpy as jnp
import numpy as np
from jax import lax

D = 2048
F = 768
TOPK = 8
TOK_DEV = 16
EXPERTS = 16
TOKENS = 256
CAP = 16
N_EP = 16


def levels(key, dims, cuts, low, largest):
    level, own = 1.0, jax.random.fold_in(key, 6)
    for position, shards_of in cuts:
        draws = jnp.exp(jax.random.uniform(jax.random.fold_in(own, position), (shards_of,), jnp.float32, low / len(cuts), largest / len(cuts)))
        level = level * jnp.repeat(draws, dims[position] // shards_of).reshape([-1 if axis == position else 1 for axis in range(len(dims))])
    return level


def deal_out(rng, own, number, rows, number_of, top, most, slope):
    order = jax.random.permutation(rng, number_of)
    packed, common = portions_of(number_of, rows * top, most, slope, True), portions_of(number_of, rows * top, most, slope, False)
    places = jnp.arange(number_of)

    def named(sizes, offset_by):
        used = int((sizes > 0).sum())
        fixed = max(1, used // 4)
        shifted = fixed + (places - fixed + offset_by * (used - fixed)) % max(1, number_of - fixed)
        return jnp.zeros((number_of,), jnp.int32).at[order[jnp.where(places < fixed, places, shifted)]].set(jnp.asarray(sizes, jnp.int32))

    sizes = jnp.where(number % 4 == 0, named(packed, number // 4), named(common, number - number // 4 - 1))
    mixed = jax.random.permutation(jax.random.fold_in(own, 3), number_of)
    source_of, sink = mixed[0:number_of // 2 * 2:2], mixed[1:number_of // 2 * 2:2]
    slack = jnp.minimum(sizes[source_of] - 1, most - sizes[sink]) // 2
    slack = jnp.where((source_of == order[0]) | (sink == order[0]) | (sizes[sink] == 0), 0, jnp.maximum(slack, 0))
    shifted = jax.random.randint(jax.random.fold_in(own, 4), (number_of // 2,), 0, 1 << 20) % (slack + 1)
    sizes = sizes.at[source_of].add(-shifted).at[sink].add(shifted)
    members = jnp.searchsorted(jnp.cumsum(sizes), jnp.arange(rows * top), side="right").astype(jnp.int32)
    listing = members.reshape(top, rows).T
    listing = listing[jax.random.permutation(jax.random.fold_in(own, 1), rows)]
    offset_by = jax.random.randint(jax.random.fold_in(own, 2), (rows, 1), 0, top)
    return jnp.take_along_axis(listing, (jnp.arange(top)[None, :] + offset_by) % top, axis=1)


def portions_of(amount, total, limit, lean, full):
    loads = [(1 << 20) // math.isqrt(grade ** lean) + 1 for grade in range(1, amount + 1)]
    largest = limit if full else min(limit, max(-(-total // amount), total * loads[0] // sum(loads)))
    least = 1 if total - largest >= amount - 1 else 0
    given, spare = [largest] + [least] * (amount - 1), total - largest - least * (amount - 1)
    while spare > 0:
        movable = [i for i in range(1, amount) if given[i] < largest] or [i for i in range(1, amount) if given[i] < limit]
        whole, budget = sum([loads[i] for i in movable]), spare
        for i in movable:
            more = min(limit - given[i], max(1, budget * loads[i] // whole), spare)
            given[i] = given[i] + more
            spare = spare - more
    return np.array(given)


def normal_values(key, shape, scale, most, cuts=(), held_as=jnp.bfloat16):
    factor_of = levels(key, shape, cuts, -0.22, 0.18) if cuts else 1.0
    values = jax.random.normal(key, shape, jnp.float32) * scale * factor_of
    return jnp.minimum(jnp.maximum(values, -most), most).astype(held_as)


def setup_inputs(seed: int = 0, part: int = 0) -> dict:
    key_list = jax.random.split(jax.random.key(seed), 7)
    part_splits = jax.random.split(jax.random.fold_in(key_list[6], part), 7)
    tokens = normal_values(part_splits[0], (TOKENS, D), 1.0, 6.0, ((0, 16),))
    gate_up = normal_values(part_splits[1], (D, EXPERTS, 2 * F), D ** -0.5, 0.125, ((0, 16),))
    down_proj = normal_values(part_splits[2], (F, EXPERTS, D), F ** -0.5, 0.21875, ((0, 16),))
    expert_ids_keys = jax.random.split(jax.random.fold_in(part_splits[3], 1), TOKENS // TOK_DEV)
    expert_ids_turns = jax.random.permutation(jax.random.fold_in(part_splits[3], 3), TOKENS // TOK_DEV)
    expert_ids = jax.vmap(lambda own, number: deal_out(jax.random.fold_in(part_splits[3], 2), own, number, TOK_DEV, EXPERTS, TOPK, CAP, 1))(expert_ids_keys, expert_ids_turns).reshape((TOKENS, TOPK))
    gate_weights = jnp.clip(jnp.exp(math.log(0.6) - 2.9957323 * jax.random.uniform(part_splits[4], (TOKENS, TOPK), jnp.float32) ** levels(part_splits[4], (TOKENS, TOPK), ((0, 16),), -0.2, 0.2)), 0.03, 0.6)
    owner_slot = jax.random.permutation(part_splits[5], EXPERTS).astype(jnp.int32)
    return dict(tokens=tokens, gate_up=gate_up, down_proj=down_proj, expert_ids=expert_ids, gate_weights=gate_weights, owner_slot=owner_slot)


def expert_ffn(rows, w_up, w_down):
    hidden = jnp.dot(rows, w_up, preferred_element_type=jnp.float32)
    ffn_width = w_up.shape[1] // 2
    activated = (jax.nn.silu(hidden[:, :ffn_width]) * hidden[:, ffn_width:]).astype(jnp.bfloat16)
    return jnp.dot(activated, w_down, preferred_element_type=jnp.float32).astype(jnp.bfloat16)

def column_scales(gate_up, down_proj):
    gate_scale = lax.optimization_barrier(jnp.max(jnp.abs(gate_up), axis=0)).astype(jnp.float32) * math.sqrt(gate_up.shape[0])
    down_scale = lax.optimization_barrier(jnp.max(jnp.abs(down_proj), axis=0)).astype(jnp.float32) * math.sqrt(down_proj.shape[0])
    return jnp.concatenate([gate_scale, down_scale], axis=1)

def reference(tokens, gate_up, down_proj, expert_ids, gate_weights, owner_slot):
    tok_all, model_width = tokens.shape
    top_count = expert_ids.shape[1]
    experts_all = gate_up.shape[1]
    most_rows = N_EP * CAP
    flat_ids = expert_ids.reshape(-1).astype(jnp.int32)
    ordering = jnp.argsort(flat_ids, stable=True).astype(jnp.int32)
    experts_iota = jnp.arange(experts_all, dtype=jnp.int32)
    counts = lax.optimization_barrier(jnp.sum((flat_ids[:, None] == experts_iota[None, :]).astype(jnp.int32), axis=0))
    starts = (jnp.cumsum(counts) - counts).astype(jnp.int32)
    padded = jnp.concatenate([ordering, jnp.zeros((most_rows,), jnp.int32)])
    flat_gates = gate_weights.reshape(-1)

    def visit(mixed, expert):
        picked = lax.dynamic_slice_in_dim(padded, starts[expert], most_rows)
        is_live = jnp.arange(most_rows, dtype=jnp.int32) < counts[expert]
        token_row = (picked // top_count).astype(jnp.int32)
        weighting = jnp.where(is_live, flat_gates[picked], jnp.zeros_like(flat_gates[picked]))
        rows = tokens[token_row]
        w_up = lax.dynamic_index_in_dim(gate_up, expert, 1, keepdims=False)
        w_down = lax.dynamic_index_in_dim(down_proj, expert, 1, keepdims=False)
        expert_out = expert_ffn(rows, w_up, w_down)
        mixed = mixed.at[token_row].add(weighting[:, None] * expert_out.astype(jnp.float32))
        return (mixed, None)
    mixed, ignored = lax.scan(visit, jnp.zeros((tok_all, model_width), jnp.float32), experts_iota)
    scales = column_scales(gate_up, down_proj)
    inverse = jnp.zeros((experts_all,), jnp.int32).at[owner_slot].set(experts_iota)
    return (mixed.astype(jnp.bfloat16), scales[inverse])
```

```python
import functools
import math

import jax
import jax.numpy as jnp
from jax import lax
from jax.experimental import pallas as pl
from jax.experimental.pallas import tpu as pltpu
from jax.sharding import PartitionSpec as P


def expert_block(arrived, held_up, held_down):
    hidden = jnp.einsum("rjd,djf->rjf", arrived, held_up, preferred_element_type=jnp.float32)
    ffn_width = held_up.shape[2] // 2
    activated = (jax.nn.silu(hidden[..., :ffn_width]) * hidden[..., ffn_width:]).astype(
        jnp.bfloat16
    )
    return jnp.einsum(
        "rjf,fjd->rjd", activated, held_down, preferred_element_type=jnp.float32
    ).astype(jnp.bfloat16)


def column_scales(gate_up, down_proj):
    gate_scale = jnp.max(jnp.abs(gate_up), axis=0).astype(jnp.float32) * math.sqrt(gate_up.shape[0])
    down_scale = jnp.max(jnp.abs(down_proj), axis=0).astype(jnp.float32) * math.sqrt(
        down_proj.shape[0]
    )
    return jnp.concatenate([gate_scale, down_scale], axis=1)


def shards(tokens, gate_up, down_proj, expert_ids, gate_weights, owner_slot):
    tok_rows, model_width = tokens.shape
    top_count = expert_ids.shape[1]
    slots_all = gate_up.shape[1]
    devices = lax.axis_size("ep")
    own_count = slots_all // devices
    capacity = 2 * tok_rows * top_count // slots_all
    experts_iota = jnp.arange(slots_all, dtype=jnp.int32)
    inverse = jnp.zeros((slots_all,), jnp.int32).at[owner_slot].set(experts_iota)
    flat_ids = expert_ids.reshape(-1)
    one_hot = (flat_ids[:, None] == experts_iota[None, :]).astype(jnp.int32)
    slot_rank = jnp.sum((jnp.cumsum(one_hot, axis=0) - 1) * one_hot, axis=1)
    position = slot_rank * slots_all + flat_ids
    source_rows = jnp.repeat(tokens, top_count, axis=0)
    outbox = (
        jnp.zeros((capacity * slots_all, model_width), jnp.bfloat16).at[position].set(source_rows)
    )
    outbox = outbox.reshape(capacity, slots_all, model_width)
    held_up, held_down = (
        lax.all_to_all(gate_up, "ep", split_axis=1, concat_axis=0, tiled=True),
        lax.all_to_all(down_proj, "ep", split_axis=1, concat_axis=0, tiled=True),
    )
    arrived = lax.all_to_all(outbox, "ep", split_axis=1, concat_axis=0, tiled=True)
    expert_out = expert_block(arrived, held_up, held_down)
    returned = lax.all_to_all(expert_out, "ep", split_axis=0, concat_axis=1, tiled=True).reshape(
        capacity * slots_all, model_width
    )
    picked = returned[position].astype(jnp.float32).reshape(tok_rows, top_count, model_width)
    moe_out = jnp.sum(picked * gate_weights[:, :, None], axis=1).astype(jnp.bfloat16)
    scales = column_scales(held_up, held_down)
    every_row = lax.all_gather(scales, "ep", axis=0, tiled=True)
    mine = lax.dynamic_slice_in_dim(inverse, lax.axis_index("ep") * own_count, own_count)
    scales = jnp.take(every_row, mine, axis=0)
    return (moe_out, scales)


MESH = pl.DeviceIdType.MESH
F32, BF16 = jnp.float32, jnp.bfloat16
GROUPS = 4
LATERAL = 1


def orders(bits):
    across = tuple(range(bits))
    return across, across[1:] + across[:1]


def fused_kernel(
    dims, tok_ref, ids_ref, gate_ref, slot_ref, up_hbm, down_hbm, out_ref, scale_ref,
    w_ref, wt_ref, wt_in, d_ref, parcel, tok_all, turned_ref, tok_t, gates_ref, pat_ref, x_ref,
    h_ref, act_ref, spread_ref, o_ref, o_in, out32, s_pair, s_send, s_recv, *rest,
):
    m, bits = dims
    hs, hr = rest[:bits], rest[bits : 2 * bits]
    (
        os_, or_, w_sem, d_sem, wt_ssem, wt_rsem, tok_ssem, tok_rsem, scale_ssem, scale_rsem,
        pair_ssem, pair_rsem, h_ssem, h_rsem, p_ssem, p_rsem, o_ssem, o_rsem,
    ) = rest[2 * bits :]
    n = 2 * m
    me = lax.axis_index("ep")
    chip, core = me // 2, lax.rem(me, 2)
    own = tok_ref.shape[0]
    total = tok_all.shape[0]
    deep = x_ref.shape[0] * x_ref.shape[1] // slot_ref.shape[1]
    depth = deep // 2
    experts = slot_ref.shape[1]
    top = ids_ref.shape[0]
    groups, small = GROUPS, own // GROUPS
    span = m * small
    lanes = span * top
    pieces = 2 * groups
    half = w_ref.shape[1] // 2
    fl = half // n
    width = d_ref.shape[1]
    root_d, root_f = math.sqrt(deep * m), math.sqrt(half)
    tile = 256
    blocks = w_ref.shape[0] // tile

    def load_w(r):
        rows = pl.ds(pl.multiple_of(r * tile, tile), tile)
        return pltpu.make_async_copy(up_hbm.at[rows, :], w_ref.at[rows, :], w_sem.at[r])

    load_d = pltpu.make_async_copy(down_hbm, d_ref, d_sem.at[0])
    for r in range(blocks):
        load_w(r).start()
    load_d.start()

    def remote(src, dst, ssem, rsem, peer):
        return pltpu.make_async_remote_copy(
            src_ref=src, dst_ref=dst, send_sem=ssem, recv_sem=rsem,
            device_id={"ep": peer}, device_id_type=MESH,
        )

    mate = 2 * chip + 1 - core

    def across(i):
        return lax.rem(chip + i, m)

    barrier = pltpu.get_barrier_semaphore()
    for i in range(1, n):
        pl.semaphore_signal(
            barrier, inc=1, device_id={"ep": lax.rem(me + i, n)}, device_id_type=MESH
        )

    gates = gate_ref[...]
    facts = [ids_ref[...].astype(F32)]
    for _ in range(3):
        high = gates.astype(BF16).astype(F32)
        facts.append(high)
        gates = gates - high
    facts.append(jnp.zeros((128 - 4 * top, own), F32))
    same = (
        lax.broadcasted_iota(jnp.int32, (own, own), 0)
        == lax.broadcasted_iota(jnp.int32, (own, own), 1)
    ).astype(F32).astype(BF16)
    meta = lax.dot_general(
        same, jnp.concatenate(facts, axis=0).astype(BF16), (((1,), (1,)), ((), ())),
        preferred_element_type=F32,
    ).astype(BF16)
    for j in range(m):
        parcel[j, :, 0:deep] = tok_ref[:, j * deep : (j + 1) * deep]
        parcel[j, :, deep : deep + 128] = meta
    pl.semaphore_wait(barrier, n - 1)

    mine = pl.ds(pl.multiple_of(me * own, own), own)

    def tok_copy(i):
        peer = lax.rem(me + i, n)
        return remote(
            parcel.at[peer // 2], tok_all.at[mine, :], tok_ssem.at[i], tok_rsem.at[i], peer
        )

    def scale_copy(i):
        to = 2 * across(i) + core
        return remote(s_send.at[to], s_recv.at[chip], scale_ssem.at[i], scale_rsem.at[i], to)

    def wt_copy(r):
        at = pl.ds(pl.multiple_of(r * tile, tile), tile)
        return remote(
            wt_ref.at[1 - core, :, at], wt_in.at[:, at], wt_ssem.at[r], wt_rsem.at[r], mate
        )

    pair_copy = remote(s_pair.at[0], s_pair.at[1], pair_ssem.at[0], pair_rsem.at[0], mate)

    for i in range(1, n):
        tok_copy(i).start()
    tok_all[mine, :] = parcel[chip]

    @pl.loop(0, blocks)
    def _(r):
        load_w(r).wait()
        rows = pl.ds(pl.multiple_of(r * tile, tile), tile)
        for at in range(0, 2 * half, tile):
            turned = w_ref[rows, at : at + tile].T
            part, first = at // half, at % half
            done = 0
            while done < tile:
                device, f = (first + done) // fl, (first + done) % fl
                count = min(fl - f, tile - done)
                to = (device // 2) * 2 * fl + part * fl + f
                wt_ref[device % 2, to : to + count, rows] = turned[done : done + count]
                done += count
        wt_copy(r).start()

    act_ref[...] = jnp.zeros_like(act_ref)
    spread_ref[...] = (
        lax.broadcasted_iota(jnp.int32, spread_ref.shape, 0)
        == lax.broadcasted_iota(jnp.int32, spread_ref.shape, 1) // experts
    ).astype(F32).astype(BF16)
    for i in range(1, n):
        tok_copy(i).wait_recv()
    turned_ref[...] = tok_all[...].T
    load_d.wait()

    def peer_of(bit):
        step = 1 << bit
        return 2 * (chip + step * (1 - 2 * lax.rem(chip // step, 2))) + core

    def h_copy(q, s, order):
        return remote(
            hs[s].at[q], hr[s].at[q], h_ssem.at[s, q], h_rsem.at[s, q], peer_of(order[s])
        )

    def h_rows(q, j, part):
        at = pl.multiple_of(j * 2 * fl + part * fl, 16)
        return h_ref[q, pl.ds(at, fl), :]

    def h_sum(q, j, s, part, order):
        total_ = h_rows(q, j, part)
        for prior in range(s):
            at = 0
            for i, bit in enumerate(sorted(order[prior + 1 :])):
                at = at + (lax.rem(j // (1 << bit), 2) << i)
            total_ += hr[prior][q, at, pl.ds(part * fl, fl), :].astype(F32)
        return total_

    def h_send(q, s, order):
        if s > 0:
            h_copy(q, s - 1, order).wait_recv()
        base = (1 - lax.rem(chip // (1 << order[s]), 2)) * (1 << order[s])
        for bit in order[:s]:
            base = base + lax.rem(chip // (1 << bit), 2) * (1 << bit)
        left = sorted(order[s + 1 :])
        for at in range(1 << len(left)):
            j = base + sum(((at >> i) & 1) << bit for i, bit in enumerate(left))
            for part in range(2):
                hs[s][q, at, pl.ds(part * fl, fl), :] = h_sum(q, j, s, part, order).astype(BF16)
        h_copy(q, s, order).start()

    def either(q, run):
        usual, lateral = orders(bits)

        @pl.when(q == LATERAL)
        def _():
            run(lateral)

        @pl.when(q != LATERAL)
        def _():
            run(usual)

    def product(q):
        p, g = lax.rem(q, 2), q // 2
        lane = lax.broadcasted_iota(jnp.int32, (1, lanes), 1)
        spot = lax.rem(lane, span)
        source = (2 * (spot // small) + p) * own + g * small + lax.rem(spot, small)
        pick = (
            lax.broadcasted_iota(jnp.int32, (total, lanes), 0) == source
        ).astype(F32).astype(BF16)
        in_slot = lax.broadcasted_iota(jnp.int32, (top, lanes), 0) == lane // span
        picked = jnp.dot(turned_ref[...], pick, preferred_element_type=F32)
        tok_t[...] = picked[0:deep]
        facts = picked[deep : deep + 4 * top]
        gate_sum = facts[top : 2 * top] + facts[2 * top : 3 * top] + facts[3 * top : 4 * top]
        ids = jnp.sum(jnp.where(in_slot, facts[0:top], 0.0), axis=0, keepdims=True)
        gates_ref[q] = jnp.sum(jnp.where(in_slot, gate_sum, 0.0), axis=0, keepdims=True)
        mask = ids == lax.broadcasted_iota(jnp.int32, (experts, lanes), 0).astype(F32)
        wide = jnp.broadcast_to(ids, (128, lanes)).T
        marks = lax.rem(lax.broadcasted_iota(jnp.int32, (lanes, 128), 1), experts).astype(F32)
        pat_ref[q] = (wide == marks).astype(F32)

        @pl.loop(0, depth // 8)
        def _(block):
            for side in range(2):
                for inner in range(8):
                    d = block * 8 + inner
                    row = jnp.where(mask, tok_t[pl.ds(side * depth + d, 1), :], 0.0)
                    at = pl.ds(pl.multiple_of(d * experts, experts), experts)
                    x_ref[side, at, :] = row.astype(BF16)


        h_ref[q] = jnp.dot(
            wt_ref[core], x_ref[core], preferred_element_type=F32
        ) + jnp.dot(wt_in[...], x_ref[1 - core], preferred_element_type=F32)

    def p_copy(q):
        return remote(o_ref.at[q], o_in.at[q // 2], p_ssem.at[q // 2], p_rsem.at[q // 2], mate)

    def o_copy(g, i):
        peer = across(i)
        return remote(
            os_.at[g, peer], or_.at[g, chip], o_ssem.at[g, i], o_rsem.at[g, i], 2 * peer + core
        )

    def h_final(q, order):
        h_copy(q, bits - 1, order).wait_recv()
        gate = h_sum(q, chip, bits, 0, order)
        act = gate / (1.0 + jnp.exp(-gate)) * h_sum(q, chip, bits, 1, order)
        act_ref[0:fl, :] = act * gates_ref[q]

    def o_product(q):
        spread = jnp.dot(
            act_ref[...].T.astype(BF16), spread_ref[...], preferred_element_type=F32
        )
        folded = []
        for at in range(0, fl * experts, 128):
            sum_ = spread[0:span, at : at + 128] * pat_ref[q, 0:span]
            for k in range(1, top):
                rows = slice(k * span, (k + 1) * span)
                sum_ += spread[rows, at : at + 128] * pat_ref[q, rows]
            folded.append(sum_.astype(BF16))
        placed = jnp.concatenate(folded, axis=1)
        o_ref[q] = jnp.dot(placed, d_ref[...], preferred_element_type=F32)

        @pl.when(core != lax.rem(q, 2))
        def _():
            p_copy(q).start()

    def o_send(q):
        g = q // 2

        @pl.when(core == lax.rem(q, 2))
        def _():
            p_copy(q).wait_recv()
            both = o_ref[q] + o_in[g]
            for j in range(m):
                os_[g, j] = both[j * small : (j + 1) * small].astype(BF16)
            for i in range(1, m):
                o_copy(g, i).start()

    def o_final(q):
        g = q // 2

        @pl.when(core == lax.rem(q, 2))
        def _():
            for i in range(1, m):
                o_copy(g, i).wait_recv()
            total_ = os_[g, chip].astype(F32)
            for i in range(1, m):
                total_ += or_[g, across(i)].astype(F32)
            out32[g] = total_

    def scales_in():
        def up_max(r, best):
            rows = pl.ds(pl.multiple_of(r * experts, experts), experts)
            return jnp.maximum(best, jnp.abs(w_ref[rows, :]))

        def down_max(r, best):
            rows = pl.ds(pl.multiple_of(r * experts, experts), experts)
            return jnp.maximum(best, jnp.abs(d_ref[rows, :]))

        choose = (
            lax.broadcasted_iota(jnp.int32, (experts, experts), 0)
            == jnp.broadcast_to(slot_ref[...], (experts, experts))
        ).astype(F32).astype(BF16)
        best = lax.fori_loop(0, depth, up_max, jnp.zeros((experts, 2 * half), BF16))
        s_pair[0, :, pl.ds(0, 2 * half)] = jnp.dot(
            choose, best, preferred_element_type=F32
        ).astype(BF16)
        best = lax.fori_loop(0, fl, down_max, jnp.zeros((experts, width), BF16))
        s_pair[0, :, pl.ds(2 * half, width)] = jnp.dot(
            choose, best, preferred_element_type=F32
        ).astype(BF16)
        pair_copy.start()

    def scales_out():
        pair_copy.wait_recv()
        best = jnp.maximum(s_pair[0].astype(F32), s_pair[1].astype(F32))
        for slot in range(experts):
            s_send[slot] = best[slot : slot + 1]
        for i in range(1, m):
            scale_copy(i).start()

    for r in range(blocks):
        wt_copy(r).wait_recv()
    lags = [0] + [s + 1 for s in range(1, bits + 1)]
    late = lags[bits]

    @pl.loop(0, pieces + late + 2)
    def _(step):
        @pl.when(step < pieces)
        def _():
            product(step)
            either(step, functools.partial(h_send, step, 0))

        for s in range(1, bits):
            @pl.when((step >= lags[s]) & (step < pieces + lags[s]))
            def _():
                either(step - lags[s], functools.partial(h_send, step - lags[s], s))

        @pl.when((step >= late) & (step < pieces + late))
        def _():
            either(step - late, functools.partial(h_final, step - late))
            o_product(step - late)

        @pl.when((step >= late + 1) & (step < pieces + late + 1))
        def _():
            o_send(step - late - 1)

        @pl.when(step >= late + 2)
        def _():
            o_final(step - late - 2)

        @pl.when(step == pieces)
        def _():
            scales_in()

        @pl.when(step == pieces + 1)
        def _():
            scales_out()

    out_ref[...] = jnp.concatenate([out32[g] for g in range(groups)], axis=0).astype(BF16)
    for i in range(1, m):
        scale_copy(i).wait_recv()
    best = s_send[me]
    for i in range(1, m):
        best = jnp.maximum(best, s_recv[across(i)])
    scale_ref[:, pl.ds(0, 2 * half)] = best[:, : 2 * half] * root_d
    scale_ref[:, pl.ds(2 * half, width)] = best[:, 2 * half :] * root_f
    for i in range(1, n):
        tok_copy(i).wait_send()
    for i in range(1, m):
        scale_copy(i).wait_send()
    for r in range(blocks):
        wt_copy(r).wait_send()
    pair_copy.wait_send()

    @pl.loop(0, pieces)
    def _(q):
        for s in range(bits):
            h_copy(q, s, orders(bits)[0]).wait_send()

    @pl.loop(0, groups)
    def _(g):
        p_copy(2 * g + 1 - core).wait_send()
        for i in range(1, m):
            o_copy(g, i).wait_send()


def fused(tokens, gate_up, down_proj, expert_ids, gate_weights, owner_slot):
    m = lax.axis_size("ep") // 2
    bits = m.bit_length() - 1
    own, width = tokens.shape
    depth, experts, both = gate_up.shape
    fl = down_proj.shape[0]
    top = expert_ids.shape[1]
    total = own * 2 * m
    small = own // GROUPS
    span = m * small
    lanes = span * top
    pieces = 2 * GROUPS
    blocks = depth * experts // 256
    vmem = pl.BlockSpec(memory_space=pltpu.VMEM)
    hbm = pl.BlockSpec(memory_space=pl.ANY)
    bufs = [pltpu.VMEM((pieces, m >> (s + 1), 2 * fl, lanes), BF16) for s in range(bits)]
    dma = pltpu.SemaphoreType.DMA
    return pl.pallas_call(
        functools.partial(fused_kernel, (m, bits)),
        out_shape=(
            jax.ShapeDtypeStruct((own, width), BF16),
            jax.ShapeDtypeStruct((1, both + width), F32),
        ),
        in_specs=[vmem, vmem, vmem, vmem, hbm, hbm],
        out_specs=(vmem, vmem),
        scratch_shapes=[
            pltpu.VMEM((depth * experts, both), BF16),
            pltpu.VMEM((2, both // 2, depth * experts), BF16),
            pltpu.VMEM((both // 2, depth * experts), BF16),
            pltpu.VMEM((fl * experts, width), BF16),
            pltpu.VMEM((m, own, 2 * depth + 128), BF16),
            pltpu.VMEM((total, 2 * depth + 128), BF16),
            pltpu.VMEM((2 * depth + 128, total), BF16),
            pltpu.VMEM((2 * depth, lanes), F32),
            pltpu.VMEM((pieces, 1, lanes), F32),
            pltpu.VMEM((pieces, lanes, 128), F32),
            pltpu.VMEM((2, depth * experts, lanes), BF16),
            pltpu.VMEM((pieces, both // 2, lanes), F32),
            pltpu.VMEM((128, lanes), F32),
            pltpu.VMEM((128, fl * experts), BF16),
            pltpu.VMEM((pieces, span, width), F32),
            pltpu.VMEM((GROUPS, span, width), F32),
            pltpu.VMEM((GROUPS, small, width), F32),
            pltpu.VMEM((2, experts, both + width), BF16),
            pltpu.VMEM((experts, 1, both + width), F32),
            pltpu.VMEM((m, 1, both + width), F32),
            *bufs, *bufs,
            pltpu.VMEM((GROUPS, m, small, width), BF16),
            pltpu.VMEM((GROUPS, m, small, width), BF16),
            dma((blocks,)), dma((1,)), dma((blocks,)), dma((blocks,)),
            dma((2 * m,)), dma((2 * m,)), dma((m,)), dma((m,)), dma((1,)), dma((1,)),
            dma((bits, pieces)), dma((bits, pieces)), dma((GROUPS,)), dma((GROUPS,)),
            dma((GROUPS, m)), dma((GROUPS, m)),
        ],
        compiler_params=pltpu.CompilerParams(
            collective_id=0, has_side_effects=True, vmem_limit_bytes=60 * 2**20
        ),
    )(
        tokens,
        expert_ids.T,
        gate_weights.T,
        owner_slot.reshape(1, experts),
        gate_up.reshape(depth * experts, both),
        down_proj.reshape(fl * experts, width),
    )


def layer(tokens, gate_up, down_proj, expert_ids, gate_weights, owner_slot):
    n = lax.axis_size("ep")
    own = tokens.shape[0]
    depth, experts, both = gate_up.shape
    partials = n * own * expert_ids.shape[1] * both
    aligned = (
        n & (n - 1) == 0 and depth % 128 == 0 and experts == n and experts % 16 == 0
        and down_proj.shape[0] % 16 == 0 and down_proj.shape[0] <= 128 and own % 16 == 0
        and n >= 4 and n * own * expert_ids.shape[1] % (256 * GROUPS) == 0
    )
    args = (tokens, gate_up, down_proj, expert_ids, gate_weights, owner_slot)
    return fused(*args) if aligned and partials <= gate_up.size else shards(*args)


def solution(mesh):
    in_specs = (
        P(("parts", "ep"), None),
        P(("parts", "ep"), None, None),
        P(("parts", "ep"), None, None),
        P(("parts", "ep"), None),
        P(("parts", "ep"), None),
        P("parts"),
    )
    out_specs = (P(("parts", "ep"), None), P(("parts", "ep"), None))
    return jax.shard_map(layer, mesh=mesh, in_specs=in_specs, out_specs=out_specs, check_vma=False)
```

```python
import functools
import math

import jax
import jax.numpy as jnp
from jax import lax
from jax.experimental import pallas as pl
from jax.experimental.pallas import tpu as pltpu
from jax.sharding import PartitionSpec as P


def expert_block(arrived, held_up, held_down):
    hidden = jnp.einsum("rjd,djf->rjf", arrived, held_up, preferred_element_type=jnp.float32)
    ffn_width = held_up.shape[2] // 2
    activated = (jax.nn.silu(hidden[..., :ffn_width]) * hidden[..., ffn_width:]).astype(
        jnp.bfloat16
    )
    return jnp.einsum(
        "rjf,fjd->rjd", activated, held_down, preferred_element_type=jnp.float32
    ).astype(jnp.bfloat16)


def column_scales(gate_up, down_proj):
    gate_scale = jnp.max(jnp.abs(gate_up), axis=0).astype(jnp.float32) * math.sqrt(gate_up.shape[0])
    down_scale = jnp.max(jnp.abs(down_proj), axis=0).astype(jnp.float32) * math.sqrt(
        down_proj.shape[0]
    )
    return jnp.concatenate([gate_scale, down_scale], axis=1)


def shards(tokens, gate_up, down_proj, expert_ids, gate_weights, owner_slot):
    tok_rows, model_width = tokens.shape
    top_count = expert_ids.shape[1]
    slots_all = gate_up.shape[1]
    devices = lax.axis_size("ep")
    own_count = slots_all // devices
    capacity = 2 * tok_rows * top_count // slots_all
    experts_iota = jnp.arange(slots_all, dtype=jnp.int32)
    inverse = jnp.zeros((slots_all,), jnp.int32).at[owner_slot].set(experts_iota)
    flat_ids = expert_ids.reshape(-1)
    one_hot = (flat_ids[:, None] == experts_iota[None, :]).astype(jnp.int32)
    slot_rank = jnp.sum((jnp.cumsum(one_hot, axis=0) - 1) * one_hot, axis=1)
    position = slot_rank * slots_all + flat_ids
    source_rows = jnp.repeat(tokens, top_count, axis=0)
    outbox = (
        jnp.zeros((capacity * slots_all, model_width), jnp.bfloat16).at[position].set(source_rows)
    )
    outbox = outbox.reshape(capacity, slots_all, model_width)
    held_up, held_down = (
        lax.all_to_all(gate_up, "ep", split_axis=1, concat_axis=0, tiled=True),
        lax.all_to_all(down_proj, "ep", split_axis=1, concat_axis=0, tiled=True),
    )
    arrived = lax.all_to_all(outbox, "ep", split_axis=1, concat_axis=0, tiled=True)
    expert_out = expert_block(arrived, held_up, held_down)
    returned = lax.all_to_all(expert_out, "ep", split_axis=0, concat_axis=1, tiled=True).reshape(
        capacity * slots_all, model_width
    )
    picked = returned[position].astype(jnp.float32).reshape(tok_rows, top_count, model_width)
    moe_out = jnp.sum(picked * gate_weights[:, :, None], axis=1).astype(jnp.bfloat16)
    scales = column_scales(held_up, held_down)
    every_row = lax.all_gather(scales, "ep", axis=0, tiled=True)
    mine = lax.dynamic_slice_in_dim(inverse, lax.axis_index("ep") * own_count, own_count)
    scales = jnp.take(every_row, mine, axis=0)
    return (moe_out, scales)


MESH = pl.DeviceIdType.MESH
F32, BF16 = jnp.float32, jnp.bfloat16
GROUPS = 4
LATERAL = 2


def orders(bits):
    across = tuple(range(bits))
    return across, across[1:] + across[:1]


def fused_kernel(
    dims, tok_ref, ids_ref, gate_ref, slot_ref, up_hbm, down_hbm, out_ref, scale_ref,
    w_ref, wt_ref, wt_in, d_ref, parcel, tok_all, turned_ref, tok_t, gates_ref, pat_ref, x_ref,
    h_ref, act_ref, spread_ref, o_ref, o_in, out32, s_pair, s_send, s_recv, *rest,
):
    m, bits = dims
    hs, hr = rest[:bits], rest[bits : 2 * bits]
    (
        os_, or_, w_sem, d_sem, wt_ssem, wt_rsem, tok_ssem, tok_rsem, scale_ssem, scale_rsem,
        pair_ssem, pair_rsem, h_ssem, h_rsem, p_ssem, p_rsem, o_ssem, o_rsem,
    ) = rest[2 * bits :]
    n = 2 * m
    me = lax.axis_index("ep")
    chip, core = me // 2, lax.rem(me, 2)
    own = tok_ref.shape[0]
    total = tok_all.shape[0]
    deep = x_ref.shape[0] * x_ref.shape[1] // slot_ref.shape[1]
    depth = deep // 2
    experts = slot_ref.shape[1]
    top = ids_ref.shape[0]
    groups, small = GROUPS, own // GROUPS
    span = m * small
    lanes = span * top
    pieces = 2 * groups
    half = w_ref.shape[1] // 2
    fl = half // n
    width = d_ref.shape[1]
    root_d, root_f = math.sqrt(deep * m), math.sqrt(half)
    tile = 256
    blocks = w_ref.shape[0] // tile

    def load_w(r):
        rows = pl.ds(pl.multiple_of(r * tile, tile), tile)
        return pltpu.make_async_copy(up_hbm.at[rows, :], w_ref.at[rows, :], w_sem.at[r])

    load_d = pltpu.make_async_copy(down_hbm, d_ref, d_sem.at[0])
    for r in range(blocks):
        load_w(r).start()
    load_d.start()

    def remote(src, dst, ssem, rsem, peer):
        return pltpu.make_async_remote_copy(
            src_ref=src, dst_ref=dst, send_sem=ssem, recv_sem=rsem,
            device_id={"ep": peer}, device_id_type=MESH,
        )

    mate = 2 * chip + 1 - core

    def across(i):
        return lax.rem(chip + i, m)

    barrier = pltpu.get_barrier_semaphore()
    for i in range(1, n):
        pl.semaphore_signal(
            barrier, inc=1, device_id={"ep": lax.rem(me + i, n)}, device_id_type=MESH
        )

    gates = gate_ref[...]
    facts = [ids_ref[...].astype(F32)]
    for _ in range(3):
        high = gates.astype(BF16).astype(F32)
        facts.append(high)
        gates = gates - high
    facts.append(jnp.zeros((128 - 4 * top, own), F32))
    same = (
        lax.broadcasted_iota(jnp.int32, (own, own), 0)
        == lax.broadcasted_iota(jnp.int32, (own, own), 1)
    ).astype(F32).astype(BF16)
    meta = lax.dot_general(
        same, jnp.concatenate(facts, axis=0).astype(BF16), (((1,), (1,)), ((), ())),
        preferred_element_type=F32,
    ).astype(BF16)
    for j in range(m):
        parcel[j, :, 0:deep] = tok_ref[:, j * deep : (j + 1) * deep]
        parcel[j, :, deep : deep + 128] = meta
    pl.semaphore_wait(barrier, n - 1)

    mine = pl.ds(pl.multiple_of(me * own, own), own)

    def tok_copy(i):
        peer = lax.rem(me + i, n)
        return remote(
            parcel.at[peer // 2], tok_all.at[mine, :], tok_ssem.at[i], tok_rsem.at[i], peer
        )

    def scale_copy(i):
        to = 2 * across(i) + core
        return remote(s_send.at[to], s_recv.at[chip], scale_ssem.at[i], scale_rsem.at[i], to)

    def wt_copy(r):
        at = pl.ds(pl.multiple_of(r * tile, tile), tile)
        return remote(
            wt_ref.at[1 - core, :, at], wt_in.at[:, at], wt_ssem.at[r], wt_rsem.at[r], mate
        )

    pair_copy = remote(s_pair.at[0], s_pair.at[1], pair_ssem.at[0], pair_rsem.at[0], mate)

    for i in range(1, n):
        tok_copy(i).start()
    tok_all[mine, :] = parcel[chip]

    def largest(ref, first, count, best):
        for i in range(count):
            rows = pl.ds(pl.multiple_of(first + i * experts, experts), experts)
            best = jnp.maximum(best, jnp.abs(ref[rows, :]))
        return best

    def prepare(r, best):
        load_w(r).wait()
        rows = pl.ds(pl.multiple_of(r * tile, tile), tile)
        for at in range(0, 2 * half, tile):
            turned = w_ref[rows, at : at + tile].T
            part, first = at // half, at % half
            done = 0
            while done < tile:
                device, f = (first + done) // fl, (first + done) % fl
                count = min(fl - f, tile - done)
                to = (device // 2) * 2 * fl + part * fl + f
                wt_ref[device % 2, to : to + count, rows] = turned[done : done + count]
                done += count
        wt_copy(r).start()
        return largest(w_ref, r * tile, tile // experts, best)

    choose = (
        lax.broadcasted_iota(jnp.int32, (experts, experts), 0)
        == jnp.broadcast_to(slot_ref[...], (experts, experts))
    ).astype(F32).astype(BF16)
    best = lax.fori_loop(0, blocks, prepare, jnp.zeros((experts, 2 * half), BF16))
    s_pair[0, :, pl.ds(0, 2 * half)] = jnp.dot(
        choose, best, preferred_element_type=F32
    ).astype(BF16)
    load_d.wait()
    best = lax.fori_loop(
        0, fl // 8, lambda r, held: largest(d_ref, r * 8 * experts, 8, held),
        jnp.zeros((experts, width), BF16),
    )
    s_pair[0, :, pl.ds(2 * half, width)] = jnp.dot(
        choose, best, preferred_element_type=F32
    ).astype(BF16)
    pair_copy.start()

    act_ref[...] = jnp.zeros_like(act_ref)
    spread_ref[...] = (
        lax.broadcasted_iota(jnp.int32, spread_ref.shape, 0)
        == lax.broadcasted_iota(jnp.int32, spread_ref.shape, 1) // experts
    ).astype(F32).astype(BF16)
    for i in range(1, n):
        tok_copy(i).wait_recv()
    turned_ref[...] = tok_all[...].T

    def peer_of(bit):
        step = 1 << bit
        return 2 * (chip + step * (1 - 2 * lax.rem(chip // step, 2))) + core

    def h_copy(q, s, order):
        return remote(
            hs[s].at[q], hr[s].at[q], h_ssem.at[s, q], h_rsem.at[s, q], peer_of(order[s])
        )

    def h_rows(q, j, part):
        at = pl.multiple_of(j * 2 * fl + part * fl, 16)
        return h_ref[q, pl.ds(at, fl), :]

    def h_sum(q, j, s, part, order):
        total_ = h_rows(q, j, part)
        for prior in range(s):
            at = 0
            for i, bit in enumerate(sorted(order[prior + 1 :])):
                at = at + (lax.rem(j // (1 << bit), 2) << i)
            total_ += hr[prior][q, at, pl.ds(part * fl, fl), :].astype(F32)
        return total_

    def h_send(q, s, order):
        if s > 0:
            h_copy(q, s - 1, order).wait_recv()
        base = (1 - lax.rem(chip // (1 << order[s]), 2)) * (1 << order[s])
        for bit in order[:s]:
            base = base + lax.rem(chip // (1 << bit), 2) * (1 << bit)
        left = sorted(order[s + 1 :])
        for at in range(1 << len(left)):
            j = base + sum(((at >> i) & 1) << bit for i, bit in enumerate(left))
            for part in range(2):
                hs[s][q, at, pl.ds(part * fl, fl), :] = h_sum(q, j, s, part, order).astype(BF16)
        h_copy(q, s, order).start()

    def either(q, run):
        usual, lateral = orders(bits)

        @pl.when(q == LATERAL)
        def _():
            run(lateral)

        @pl.when(q != LATERAL)
        def _():
            run(usual)

    def build(q):
        p, g = lax.rem(q, 2), q // 2
        lane = lax.broadcasted_iota(jnp.int32, (1, lanes), 1)
        spot = lax.rem(lane, span)
        source = (2 * (spot // small) + p) * own + g * small + lax.rem(spot, small)
        pick = (
            lax.broadcasted_iota(jnp.int32, (total, lanes), 0) == source
        ).astype(F32).astype(BF16)
        in_slot = lax.broadcasted_iota(jnp.int32, (top, lanes), 0) == lane // span
        picked = jnp.dot(turned_ref[...], pick, preferred_element_type=F32)
        tok_t[...] = picked[0:deep]
        facts = picked[deep : deep + 4 * top]
        gate_sum = facts[top : 2 * top] + facts[2 * top : 3 * top] + facts[3 * top : 4 * top]
        ids = jnp.sum(jnp.where(in_slot, facts[0:top], 0.0), axis=0, keepdims=True)
        gates_ref[q] = jnp.sum(jnp.where(in_slot, gate_sum, 0.0), axis=0, keepdims=True)
        mask = ids == lax.broadcasted_iota(jnp.int32, (experts, lanes), 0).astype(F32)
        wide = jnp.broadcast_to(ids, (128, lanes)).T
        marks = lax.rem(lax.broadcasted_iota(jnp.int32, (lanes, 128), 1), experts).astype(F32)
        pat_ref[q] = (wide == marks).astype(F32)

        @pl.loop(0, depth // 8)
        def _(block):
            for side in range(2):
                for inner in range(8):
                    d = block * 8 + inner
                    row = jnp.where(mask, tok_t[pl.ds(side * depth + d, 1), :], 0.0)
                    at = pl.ds(pl.multiple_of(d * experts, experts), experts)
                    x_ref[side, at, :] = row.astype(BF16)


    def product(q):
        h_ref[q] = jnp.dot(
            wt_ref[core], x_ref[core], preferred_element_type=F32
        ) + jnp.dot(wt_in[...], x_ref[1 - core], preferred_element_type=F32)

    def p_copy(q):
        return remote(o_ref.at[q], o_in.at[q // 2], p_ssem.at[q // 2], p_rsem.at[q // 2], mate)

    def o_copy(g, i):
        peer = across(i)
        return remote(
            os_.at[g, peer], or_.at[g, chip], o_ssem.at[g, i], o_rsem.at[g, i], 2 * peer + core
        )

    def h_final(q, order):
        h_copy(q, bits - 1, order).wait_recv()
        gate = h_sum(q, chip, bits, 0, order)
        act = gate / (1.0 + jnp.exp(-gate)) * h_sum(q, chip, bits, 1, order)
        act_ref[0:fl, :] = act * gates_ref[q]

    def o_product(q):
        spread = jnp.dot(
            act_ref[...].T.astype(BF16), spread_ref[...], preferred_element_type=F32
        )
        folded = []
        for at in range(0, fl * experts, 128):
            sum_ = spread[0:span, at : at + 128] * pat_ref[q, 0:span]
            for k in range(1, top):
                rows = slice(k * span, (k + 1) * span)
                sum_ += spread[rows, at : at + 128] * pat_ref[q, rows]
            folded.append(sum_.astype(BF16))
        placed = jnp.concatenate(folded, axis=1)
        o_ref[q] = jnp.dot(placed, d_ref[...], preferred_element_type=F32)

        @pl.when(core != lax.rem(q, 2))
        def _():
            p_copy(q).start()

    def o_send(q):
        g = q // 2

        @pl.when(core == lax.rem(q, 2))
        def _():
            p_copy(q).wait_recv()
            both = o_ref[q] + o_in[g]
            for j in range(m):
                os_[g, j] = both[j * small : (j + 1) * small].astype(BF16)
            for i in range(1, m):
                o_copy(g, i).start()

    def o_final(q):
        g = q // 2

        @pl.when(core == lax.rem(q, 2))
        def _():
            for i in range(1, m):
                o_copy(g, i).wait_recv()
            total_ = os_[g, chip].astype(F32)
            for i in range(1, m):
                total_ += or_[g, across(i)].astype(F32)
            out32[g] = total_

    def scales_out():
        pair_copy.wait_recv()
        best = jnp.maximum(s_pair[0].astype(F32), s_pair[1].astype(F32))
        for slot in range(experts):
            s_send[slot] = best[slot : slot + 1]
        for i in range(1, m):
            scale_copy(i).start()

    build(0)
    scales_out()
    for r in range(blocks):
        wt_copy(r).wait_recv()
    lags = [0] + [2 * s for s in range(1, bits + 1)]
    late = lags[bits]

    @pl.loop(0, pieces + late + 1)
    def _(step):
        @pl.when(step < pieces)
        def _():
            product(step)
            either(step, functools.partial(h_send, step, 0))

        @pl.when(step < pieces - 1)
        def _():
            build(step + 1)

        for s in range(1, bits):
            @pl.when((step >= lags[s]) & (step < pieces + lags[s]))
            def _():
                either(step - lags[s], functools.partial(h_send, step - lags[s], s))

        @pl.when((step >= late) & (step < pieces + late))
        def _():
            either(step - late, functools.partial(h_final, step - late))
            o_product(step - late)

        @pl.when((step >= late + 1) & (step < pieces + late + 1))
        def _():
            o_send(step - late - 1)

    @pl.loop(0, pieces)
    def _(q):
        o_final(q)

    out_ref[...] = jnp.concatenate([out32[g] for g in range(groups)], axis=0).astype(BF16)
    for i in range(1, m):
        scale_copy(i).wait_recv()
    best = s_send[me]
    for i in range(1, m):
        best = jnp.maximum(best, s_recv[across(i)])
    scale_ref[:, pl.ds(0, 2 * half)] = best[:, : 2 * half] * root_d
    scale_ref[:, pl.ds(2 * half, width)] = best[:, 2 * half :] * root_f
    for i in range(1, n):
        tok_copy(i).wait_send()
    for i in range(1, m):
        scale_copy(i).wait_send()
    for r in range(blocks):
        wt_copy(r).wait_send()
    pair_copy.wait_send()

    @pl.loop(0, pieces)
    def _(q):
        for s in range(bits):
            h_copy(q, s, orders(bits)[0]).wait_send()

    @pl.loop(0, groups)
    def _(g):
        p_copy(2 * g + 1 - core).wait_send()
        for i in range(1, m):
            o_copy(g, i).wait_send()


def fused(tokens, gate_up, down_proj, expert_ids, gate_weights, owner_slot):
    m = lax.axis_size("ep") // 2
    bits = m.bit_length() - 1
    own, width = tokens.shape
    depth, experts, both = gate_up.shape
    fl = down_proj.shape[0]
    top = expert_ids.shape[1]
    total = own * 2 * m
    small = own // GROUPS
    span = m * small
    lanes = span * top
    pieces = 2 * GROUPS
    blocks = depth * experts // 256
    vmem = pl.BlockSpec(memory_space=pltpu.VMEM)
    hbm = pl.BlockSpec(memory_space=pl.ANY)
    bufs = [pltpu.VMEM((pieces, m >> (s + 1), 2 * fl, lanes), BF16) for s in range(bits)]
    dma = pltpu.SemaphoreType.DMA
    return pl.pallas_call(
        functools.partial(fused_kernel, (m, bits)),
        out_shape=(
            jax.ShapeDtypeStruct((own, width), BF16),
            jax.ShapeDtypeStruct((1, both + width), F32),
        ),
        in_specs=[vmem, vmem, vmem, vmem, hbm, hbm],
        out_specs=(vmem, vmem),
        scratch_shapes=[
            pltpu.VMEM((depth * experts, both), BF16),
            pltpu.VMEM((2, both // 2, depth * experts), BF16),
            pltpu.VMEM((both // 2, depth * experts), BF16),
            pltpu.VMEM((fl * experts, width), BF16),
            pltpu.VMEM((m, own, 2 * depth + 128), BF16),
            pltpu.VMEM((total, 2 * depth + 128), BF16),
            pltpu.VMEM((2 * depth + 128, total), BF16),
            pltpu.VMEM((2 * depth, lanes), F32),
            pltpu.VMEM((pieces, 1, lanes), F32),
            pltpu.VMEM((pieces, lanes, 128), F32),
            pltpu.VMEM((2, depth * experts, lanes), BF16),
            pltpu.VMEM((pieces, both // 2, lanes), F32),
            pltpu.VMEM((128, lanes), F32),
            pltpu.VMEM((128, fl * experts), BF16),
            pltpu.VMEM((pieces, span, width), F32),
            pltpu.VMEM((GROUPS, span, width), F32),
            pltpu.VMEM((GROUPS, small, width), F32),
            pltpu.VMEM((2, experts, both + width), BF16),
            pltpu.VMEM((experts, 1, both + width), F32),
            pltpu.VMEM((m, 1, both + width), F32),
            *bufs, *bufs,
            pltpu.VMEM((GROUPS, m, small, width), BF16),
            pltpu.VMEM((GROUPS, m, small, width), BF16),
            dma((blocks,)), dma((1,)), dma((blocks,)), dma((blocks,)),
            dma((2 * m,)), dma((2 * m,)), dma((m,)), dma((m,)), dma((1,)), dma((1,)),
            dma((bits, pieces)), dma((bits, pieces)), dma((GROUPS,)), dma((GROUPS,)),
            dma((GROUPS, m)), dma((GROUPS, m)),
        ],
        compiler_params=pltpu.CompilerParams(
            collective_id=0, has_side_effects=True, vmem_limit_bytes=60 * 2**20
        ),
    )(
        tokens,
        expert_ids.T,
        gate_weights.T,
        owner_slot.reshape(1, experts),
        gate_up.reshape(depth * experts, both),
        down_proj.reshape(fl * experts, width),
    )


def layer(tokens, gate_up, down_proj, expert_ids, gate_weights, owner_slot):
    n = lax.axis_size("ep")
    own = tokens.shape[0]
    depth, experts, both = gate_up.shape
    partials = n * own * expert_ids.shape[1] * both
    aligned = (
        n & (n - 1) == 0 and depth % 128 == 0 and experts == n and experts % 16 == 0
        and down_proj.shape[0] % 16 == 0 and down_proj.shape[0] <= 128 and own % 16 == 0
        and n >= 4 and n * own * expert_ids.shape[1] % (256 * GROUPS) == 0
    )
    args = (tokens, gate_up, down_proj, expert_ids, gate_weights, owner_slot)
    return fused(*args) if aligned and partials <= gate_up.size else shards(*args)


def solution(mesh):
    in_specs = (
        P(("parts", "ep"), None),
        P(("parts", "ep"), None, None),
        P(("parts", "ep"), None, None),
        P(("parts", "ep"), None),
        P(("parts", "ep"), None),
        P("parts"),
    )
    out_specs = (P(("parts", "ep"), None), P(("parts", "ep"), None))
    return jax.shard_map(layer, mesh=mesh, in_specs=in_specs, out_specs=out_specs, check_vma=False)
```

```python
import functools
import math

import jax
import jax.numpy as jnp
from jax import lax
from jax.experimental import pallas as pl
from jax.experimental.pallas import tpu as pltpu
from jax.sharding import PartitionSpec as P


def expert_block(arrived, held_up, held_down):
    hidden = jnp.einsum("rjd,djf->rjf", arrived, held_up, preferred_element_type=jnp.float32)
    ffn_width = held_up.shape[2] // 2
    activated = (jax.nn.silu(hidden[..., :ffn_width]) * hidden[..., ffn_width:]).astype(
        jnp.bfloat16
    )
    return jnp.einsum(
        "rjf,fjd->rjd", activated, held_down, preferred_element_type=jnp.float32
    ).astype(jnp.bfloat16)


def column_scales(gate_up, down_proj):
    gate_scale = jnp.max(jnp.abs(gate_up), axis=0).astype(jnp.float32) * math.sqrt(gate_up.shape[0])
    down_scale = jnp.max(jnp.abs(down_proj), axis=0).astype(jnp.float32) * math.sqrt(
        down_proj.shape[0]
    )
    return jnp.concatenate([gate_scale, down_scale], axis=1)


def shards(tokens, gate_up, down_proj, expert_ids, gate_weights, owner_slot):
    tok_rows, model_width = tokens.shape
    top_count = expert_ids.shape[1]
    slots_all = gate_up.shape[1]
    devices = lax.axis_size("ep")
    own_count = slots_all // devices
    capacity = 2 * tok_rows * top_count // slots_all
    experts_iota = jnp.arange(slots_all, dtype=jnp.int32)
    inverse = jnp.zeros((slots_all,), jnp.int32).at[owner_slot].set(experts_iota)
    flat_ids = expert_ids.reshape(-1)
    one_hot = (flat_ids[:, None] == experts_iota[None, :]).astype(jnp.int32)
    slot_rank = jnp.sum((jnp.cumsum(one_hot, axis=0) - 1) * one_hot, axis=1)
    position = slot_rank * slots_all + flat_ids
    source_rows = jnp.repeat(tokens, top_count, axis=0)
    outbox = (
        jnp.zeros((capacity * slots_all, model_width), jnp.bfloat16).at[position].set(source_rows)
    )
    outbox = outbox.reshape(capacity, slots_all, model_width)
    held_up, held_down = (
        lax.all_to_all(gate_up, "ep", split_axis=1, concat_axis=0, tiled=True),
        lax.all_to_all(down_proj, "ep", split_axis=1, concat_axis=0, tiled=True),
    )
    arrived = lax.all_to_all(outbox, "ep", split_axis=1, concat_axis=0, tiled=True)
    expert_out = expert_block(arrived, held_up, held_down)
    returned = lax.all_to_all(expert_out, "ep", split_axis=0, concat_axis=1, tiled=True).reshape(
        capacity * slots_all, model_width
    )
    picked = returned[position].astype(jnp.float32).reshape(tok_rows, top_count, model_width)
    moe_out = jnp.sum(picked * gate_weights[:, :, None], axis=1).astype(jnp.bfloat16)
    scales = column_scales(held_up, held_down)
    every_row = lax.all_gather(scales, "ep", axis=0, tiled=True)
    mine = lax.dynamic_slice_in_dim(inverse, lax.axis_index("ep") * own_count, own_count)
    scales = jnp.take(every_row, mine, axis=0)
    return (moe_out, scales)


MESH = pl.DeviceIdType.MESH
F32, BF16 = jnp.float32, jnp.bfloat16
GROUPS = 4
LATERAL = 2


def orders(bits):
    across = tuple(range(bits))
    return across, across[1:] + across[:1]


def fused_kernel(
    dims, tok_ref, ids_ref, gate_ref, slot_ref, up_hbm, down_hbm, out_ref, scale_ref,
    w_ref, wt_ref, wt_in, d_ref, parcel, tok_all, turned_ref, tok_t, gates_ref, pat_ref, x_ref,
    h_ref, act_ref, spread_ref, o_ref, o_in, out32, s_pair, s_send, s_recv, *rest,
):
    m, bits = dims
    hs, hr = rest[:bits], rest[bits : 2 * bits]
    (
        os_, or_, w_sem, d_sem, wt_ssem, wt_rsem, tok_ssem, tok_rsem, scale_ssem, scale_rsem,
        pair_ssem, pair_rsem, h_ssem, h_rsem, p_ssem, p_rsem, o_ssem, o_rsem,
    ) = rest[2 * bits :]
    n = 2 * m
    me = lax.axis_index("ep")
    chip, core = me // 2, lax.rem(me, 2)
    own = tok_ref.shape[0]
    total = tok_all.shape[0]
    deep = x_ref.shape[0] * x_ref.shape[1] // slot_ref.shape[1]
    depth = deep // 2
    experts = slot_ref.shape[1]
    top = ids_ref.shape[0]
    groups, small = GROUPS, own // GROUPS
    span = m * small
    lanes = span * top
    pieces = 2 * groups
    half = w_ref.shape[1] // 2
    fl = half // n
    width = d_ref.shape[1]
    root_d, root_f = math.sqrt(deep * m), math.sqrt(half)
    tile = 256
    blocks = w_ref.shape[0] // tile

    def load_w(r):
        rows = pl.ds(pl.multiple_of(r * tile, tile), tile)
        return pltpu.make_async_copy(up_hbm.at[rows, :], w_ref.at[rows, :], w_sem.at[r])

    load_d = pltpu.make_async_copy(down_hbm, d_ref, d_sem.at[0])
    for r in range(blocks):
        load_w(r).start()
    load_d.start()

    def remote(src, dst, ssem, rsem, peer):
        return pltpu.make_async_remote_copy(
            src_ref=src, dst_ref=dst, send_sem=ssem, recv_sem=rsem,
            device_id={"ep": peer}, device_id_type=MESH,
        )

    mate = 2 * chip + 1 - core

    def across(i):
        return lax.rem(chip + i, m)

    barrier = pltpu.get_barrier_semaphore()
    for i in range(1, n):
        pl.semaphore_signal(
            barrier, inc=1, device_id={"ep": lax.rem(me + i, n)}, device_id_type=MESH
        )

    gates = gate_ref[...]
    facts = [ids_ref[...].astype(F32)]
    for _ in range(3):
        high = gates.astype(BF16).astype(F32)
        facts.append(high)
        gates = gates - high
    facts.append(jnp.zeros((128 - 4 * top, own), F32))
    same = (
        lax.broadcasted_iota(jnp.int32, (own, own), 0)
        == lax.broadcasted_iota(jnp.int32, (own, own), 1)
    ).astype(F32).astype(BF16)
    meta = lax.dot_general(
        same, jnp.concatenate(facts, axis=0).astype(BF16), (((1,), (1,)), ((), ())),
        preferred_element_type=F32,
    ).astype(BF16)
    for j in range(m):
        parcel[j, :, 0:deep] = tok_ref[:, j * deep : (j + 1) * deep]
        parcel[j, :, deep : deep + 128] = meta
    pl.semaphore_wait(barrier, n - 1)

    mine = pl.ds(pl.multiple_of(me * own, own), own)

    def tok_copy(i):
        peer = lax.rem(me + i, n)
        return remote(
            parcel.at[peer // 2], tok_all.at[mine, :], tok_ssem.at[i], tok_rsem.at[i], peer
        )

    def scale_copy(i):
        to = 2 * across(i) + core
        return remote(s_send.at[to], s_recv.at[chip], scale_ssem.at[i], scale_rsem.at[i], to)

    def wt_copy(r):
        at = pl.ds(pl.multiple_of(r * tile, tile), tile)
        return remote(
            wt_ref.at[1 - core, :, at], wt_in.at[:, at], wt_ssem.at[r], wt_rsem.at[r], mate
        )

    pair_copy = remote(s_pair.at[0], s_pair.at[1], pair_ssem.at[0], pair_rsem.at[0], mate)

    for i in range(1, n):
        tok_copy(i).start()
    tok_all[mine, :] = parcel[chip]

    def largest(ref, first, count, best):
        for i in range(count):
            rows = pl.ds(pl.multiple_of(first + i * experts, experts), experts)
            best = jnp.maximum(best, jnp.abs(ref[rows, :]))
        return best

    def prepare(r, best):
        load_w(r).wait()
        rows = pl.ds(pl.multiple_of(r * tile, tile), tile)
        for at in range(0, 2 * half, tile):
            turned = w_ref[rows, at : at + tile].T
            part, first = at // half, at % half
            done = 0
            while done < tile:
                device, f = (first + done) // fl, (first + done) % fl
                count = min(fl - f, tile - done)
                to = (device // 2) * 2 * fl + part * fl + f
                wt_ref[device % 2, to : to + count, rows] = turned[done : done + count]
                done += count
        wt_copy(r).start()
        return largest(w_ref, r * tile, tile // experts, best)

    choose = (
        lax.broadcasted_iota(jnp.int32, (experts, experts), 0)
        == jnp.broadcast_to(slot_ref[...], (experts, experts))
    ).astype(F32).astype(BF16)
    best = lax.fori_loop(0, blocks, prepare, jnp.zeros((experts, 2 * half), BF16))
    s_pair[0, :, pl.ds(0, 2 * half)] = jnp.dot(
        choose, best, preferred_element_type=F32
    ).astype(BF16)
    load_d.wait()
    best = lax.fori_loop(
        0, fl // 8, lambda r, held: largest(d_ref, r * 8 * experts, 8, held),
        jnp.zeros((experts, width), BF16),
    )
    s_pair[0, :, pl.ds(2 * half, width)] = jnp.dot(
        choose, best, preferred_element_type=F32
    ).astype(BF16)
    pair_copy.start()

    act_ref[...] = jnp.zeros_like(act_ref)
    spread_ref[...] = (
        lax.broadcasted_iota(jnp.int32, spread_ref.shape, 0)
        == lax.broadcasted_iota(jnp.int32, spread_ref.shape, 1) // experts
    ).astype(F32).astype(BF16)
    for i in range(1, n):
        tok_copy(i).wait_recv()
    turned_ref[...] = tok_all[...].T

    def peer_of(bit):
        step = 1 << bit
        return 2 * (chip + step * (1 - 2 * lax.rem(chip // step, 2))) + core

    def h_copy(q, s, order):
        return remote(
            hs[s].at[q], hr[s].at[q], h_ssem.at[s, q], h_rsem.at[s, q], peer_of(order[s])
        )

    def h_rows(q, j, part):
        at = pl.multiple_of(j * 2 * fl + part * fl, 16)
        return h_ref[q, pl.ds(at, fl), :]

    def h_sum(q, j, s, part, order):
        total_ = h_rows(q, j, part)
        for prior in range(s):
            at = 0
            for i, bit in enumerate(sorted(order[prior + 1 :])):
                at = at + (lax.rem(j // (1 << bit), 2) << i)
            total_ += hr[prior][q, at, pl.ds(part * fl, fl), :].astype(F32)
        return total_

    def h_send(q, s, order):
        if s > 0:
            h_copy(q, s - 1, order).wait_recv()
        base = (1 - lax.rem(chip // (1 << order[s]), 2)) * (1 << order[s])
        for bit in order[:s]:
            base = base + lax.rem(chip // (1 << bit), 2) * (1 << bit)
        left = sorted(order[s + 1 :])
        for at in range(1 << len(left)):
            j = base + sum(((at >> i) & 1) << bit for i, bit in enumerate(left))
            for part in range(2):
                hs[s][q, at, pl.ds(part * fl, fl), :] = h_sum(q, j, s, part, order).astype(BF16)
        h_copy(q, s, order).start()

    def either(q, run):
        usual, lateral = orders(bits)

        @pl.when(q == LATERAL)
        def _():
            run(lateral)

        @pl.when(q != LATERAL)
        def _():
            run(usual)

    def build(q):
        p, g = lax.rem(q, 2), q // 2
        lane = lax.broadcasted_iota(jnp.int32, (1, lanes), 1)
        spot = lax.rem(lane, span)
        source = (2 * (spot // small) + p) * own + g * small + lax.rem(spot, small)
        pick = (
            lax.broadcasted_iota(jnp.int32, (total, lanes), 0) == source
        ).astype(F32).astype(BF16)
        in_slot = lax.broadcasted_iota(jnp.int32, (top, lanes), 0) == lane // span
        picked = jnp.dot(turned_ref[...], pick, preferred_element_type=F32)
        tok_t[...] = picked[0:deep]
        facts = picked[deep : deep + 4 * top]
        gate_sum = facts[top : 2 * top] + facts[2 * top : 3 * top] + facts[3 * top : 4 * top]
        ids = jnp.sum(jnp.where(in_slot, facts[0:top], 0.0), axis=0, keepdims=True)
        gates_ref[q] = jnp.sum(jnp.where(in_slot, gate_sum, 0.0), axis=0, keepdims=True)
        mask = ids == lax.broadcasted_iota(jnp.int32, (experts, lanes), 0).astype(F32)
        wide = jnp.broadcast_to(ids, (128, lanes)).T
        marks = lax.rem(lax.broadcasted_iota(jnp.int32, (lanes, 128), 1), experts).astype(F32)
        pat_ref[q] = (wide == marks).astype(F32)

        @pl.loop(0, depth // 8)
        def _(block):
            for side in range(2):
                for inner in range(8):
                    d = block * 8 + inner
                    row = jnp.where(mask, tok_t[pl.ds(side * depth + d, 1), :], 0.0)
                    at = pl.ds(pl.multiple_of(d * experts, experts), experts)
                    x_ref[side, at, :] = row.astype(BF16)


    def product(q):
        h_ref[q] = jnp.dot(
            wt_ref[core], x_ref[core], preferred_element_type=F32
        ) + jnp.dot(wt_in[...], x_ref[1 - core], preferred_element_type=F32)

    def p_copy(q):
        return remote(o_ref.at[q], o_in.at[q // 2], p_ssem.at[q // 2], p_rsem.at[q // 2], mate)

    def o_copy(g, i):
        peer = across(i)
        return remote(
            os_.at[g, peer], or_.at[g, chip], o_ssem.at[g, i], o_rsem.at[g, i], 2 * peer + core
        )

    def h_final(q, order):
        h_copy(q, bits - 1, order).wait_recv()
        gate = h_sum(q, chip, bits, 0, order)
        act = gate / (1.0 + jnp.exp(-gate)) * h_sum(q, chip, bits, 1, order)
        act_ref[0:fl, :] = act * gates_ref[q]

    def o_product(q):
        spread = jnp.dot(
            act_ref[...].T.astype(BF16), spread_ref[...], preferred_element_type=F32
        )
        folded = []
        for at in range(0, fl * experts, 128):
            sum_ = spread[0:span, at : at + 128] * pat_ref[q, 0:span]
            for k in range(1, top):
                rows = slice(k * span, (k + 1) * span)
                sum_ += spread[rows, at : at + 128] * pat_ref[q, rows]
            folded.append(sum_.astype(BF16))
        placed = jnp.concatenate(folded, axis=1)
        o_ref[q] = jnp.dot(placed, d_ref[...], preferred_element_type=F32)

        @pl.when(core != lax.rem(q, 2))
        def _():
            p_copy(q).start()

    def o_send(q):
        g = q // 2

        @pl.when(core == lax.rem(q, 2))
        def _():
            p_copy(q).wait_recv()
            both = o_ref[q] + o_in[g]
            for j in range(m):
                os_[g, j] = both[j * small : (j + 1) * small].astype(BF16)
            for i in range(1, m):
                o_copy(g, i).start()

    def o_final(q):
        g = q // 2

        @pl.when(core == lax.rem(q, 2))
        def _():
            for i in range(1, m):
                o_copy(g, i).wait_recv()
            total_ = os_[g, chip].astype(F32)
            for i in range(1, m):
                total_ += or_[g, across(i)].astype(F32)
            out32[g] = total_

    def scales_out():
        pair_copy.wait_recv()
        best = jnp.maximum(s_pair[0].astype(F32), s_pair[1].astype(F32))
        for slot in range(experts):
            s_send[slot] = best[slot : slot + 1]
        for i in range(1, m):
            scale_copy(i).start()

    build(0)
    scales_out()
    for r in range(blocks):
        wt_copy(r).wait_recv()
    lags = [0] + [2 * s for s in range(1, bits + 1)]
    late = lags[bits]

    @pl.loop(0, pieces + late + 1)
    def _(step):
        @pl.when(step < pieces)
        def _():
            product(step)
            either(step, functools.partial(h_send, step, 0))

        @pl.when(step < pieces - 1)
        def _():
            build(step + 1)

        for s in range(1, bits):
            @pl.when((step >= lags[s]) & (step < pieces + lags[s]))
            def _():
                either(step - lags[s], functools.partial(h_send, step - lags[s], s))

        @pl.when((step >= late) & (step < pieces + late))
        def _():
            either(step - late, functools.partial(h_final, step - late))
            o_product(step - late)

        @pl.when((step >= late + 1) & (step < pieces + late + 1))
        def _():
            o_send(step - late - 1)

    @pl.loop(0, pieces)
    def _(q):
        o_final(q)

    out_ref[...] = jnp.concatenate([out32[g] for g in range(groups)], axis=0).astype(BF16)
    for i in range(1, m):
        scale_copy(i).wait_recv()
    best = s_send[me]
    for i in range(1, m):
        best = jnp.maximum(best, s_recv[across(i)])
    scale_ref[:, pl.ds(0, 2 * half)] = best[:, : 2 * half] * root_d
    scale_ref[:, pl.ds(2 * half, width)] = best[:, 2 * half :] * root_f
    for i in range(1, n):
        tok_copy(i).wait_send()
    for i in range(1, m):
        scale_copy(i).wait_send()
    for r in range(blocks):
        wt_copy(r).wait_send()
    pair_copy.wait_send()

    @pl.loop(0, pieces)
    def _(q):
        for s in range(bits):
            h_copy(q, s, orders(bits)[0]).wait_send()

    @pl.loop(0, groups)
    def _(g):
        p_copy(2 * g + 1 - core).wait_send()
        for i in range(1, m):
            o_copy(g, i).wait_send()


def fused(tokens, gate_up, down_proj, expert_ids, gate_weights, owner_slot):
    m = lax.axis_size("ep") // 2
    bits = m.bit_length() - 1
    own, width = tokens.shape
    depth, experts, both = gate_up.shape
    fl = down_proj.shape[0]
    top = expert_ids.shape[1]
    total = own * 2 * m
    small = own // GROUPS
    span = m * small
    lanes = span * top
    pieces = 2 * GROUPS
    blocks = depth * experts // 256
    vmem = pl.BlockSpec(memory_space=pltpu.VMEM)
    hbm = pl.BlockSpec(memory_space=pl.ANY)
    bufs = [pltpu.VMEM((pieces, m >> (s + 1), 2 * fl, lanes), BF16) for s in range(bits)]
    dma = pltpu.SemaphoreType.DMA
    return pl.pallas_call(
        functools.partial(fused_kernel, (m, bits)),
        out_shape=(
            jax.ShapeDtypeStruct((own, width), BF16),
            jax.ShapeDtypeStruct((1, both + width), F32),
        ),
        in_specs=[vmem, vmem, vmem, vmem, hbm, hbm],
        out_specs=(vmem, vmem),
        scratch_shapes=[
            pltpu.VMEM((depth * experts, both), BF16),
            pltpu.VMEM((2, both // 2, depth * experts), BF16),
            pltpu.VMEM((both // 2, depth * experts), BF16),
            pltpu.VMEM((fl * experts, width), BF16),
            pltpu.VMEM((m, own, 2 * depth + 128), BF16),
            pltpu.VMEM((total, 2 * depth + 128), BF16),
            pltpu.VMEM((2 * depth + 128, total), BF16),
            pltpu.VMEM((2 * depth, lanes), F32),
            pltpu.VMEM((pieces, 1, lanes), F32),
            pltpu.VMEM((pieces, lanes, 128), F32),
            pltpu.VMEM((2, depth * experts, lanes), BF16),
            pltpu.VMEM((pieces, both // 2, lanes), F32),
            pltpu.VMEM((128, lanes), F32),
            pltpu.VMEM((128, fl * experts), BF16),
            pltpu.VMEM((pieces, span, width), F32),
            pltpu.VMEM((GROUPS, span, width), F32),
            pltpu.VMEM((GROUPS, small, width), F32),
            pltpu.VMEM((2, experts, both + width), BF16),
            pltpu.VMEM((experts, 1, both + width), F32),
            pltpu.VMEM((m, 1, both + width), F32),
            *bufs, *bufs,
            pltpu.VMEM((GROUPS, m, small, width), BF16),
            pltpu.VMEM((GROUPS, m, small, width), BF16),
            dma((blocks,)), dma((1,)), dma((blocks,)), dma((blocks,)),
            dma((2 * m,)), dma((2 * m,)), dma((m,)), dma((m,)), dma((1,)), dma((1,)),
            dma((bits, pieces)), dma((bits, pieces)), dma((GROUPS,)), dma((GROUPS,)),
            dma((GROUPS, m)), dma((GROUPS, m)),
        ],
        compiler_params=pltpu.CompilerParams(
            collective_id=0, has_side_effects=True, vmem_limit_bytes=60 * 2**20
        ),
    )(
        tokens,
        expert_ids.T,
        gate_weights.T,
        owner_slot.reshape(1, experts),
        gate_up.reshape(depth * experts, both),
        down_proj.reshape(fl * experts, width),
    )


def settle_kernel(out_ref, scale_ref, out_to, scale_to):
    out_to[...] = out_ref[...]
    scale_to[...] = scale_ref[...]


def settle(results):
    vmem = pl.BlockSpec(memory_space=pltpu.VMEM)
    return pl.pallas_call(
        settle_kernel,
        out_shape=tuple(jax.ShapeDtypeStruct(r.shape, r.dtype) for r in results),
        in_specs=[vmem, vmem],
        out_specs=(vmem, vmem),
    )(*results)


def layer(tokens, gate_up, down_proj, expert_ids, gate_weights, owner_slot):
    n = lax.axis_size("ep")
    own = tokens.shape[0]
    depth, experts, both = gate_up.shape
    partials = n * own * expert_ids.shape[1] * both
    aligned = (
        n & (n - 1) == 0 and depth % 128 == 0 and experts == n and experts % 16 == 0
        and down_proj.shape[0] % 16 == 0 and down_proj.shape[0] <= 128 and own % 16 == 0
        and n >= 4 and n * own * expert_ids.shape[1] % (256 * GROUPS) == 0
    )
    args = (tokens, gate_up, down_proj, expert_ids, gate_weights, owner_slot)
    return settle(fused(*args)) if aligned and partials <= gate_up.size else shards(*args)


def solution(mesh):
    in_specs = (
        P(("parts", "ep"), None),
        P(("parts", "ep"), None, None),
        P(("parts", "ep"), None, None),
        P(("parts", "ep"), None),
        P(("parts", "ep"), None),
        P("parts"),
    )
    out_specs = (P(("parts", "ep"), None), P(("parts", "ep"), None))
    return jax.shard_map(layer, mesh=mesh, in_specs=in_specs, out_specs=out_specs, check_vma=False)
```
